32 devices in a mesh: prow: 4 (over y, x), pcol: 8 (over z, core).
Axes of the slice: x: 2, y: 2, z: 4, core: 2. Of those that a mesh axis runs over, the one named last changes fastest.
Arguments:
- covariance: float32 [16384, 16384], P(('prow', 'pcol')), may hold values from -600 to 600, as said below
- factor_left: float32 [64, 16384], P(None, ('prow', 'pcol')), may hold values from -6 to 6
- factor_right: float32 [64, 16384], P('prow', 'pcol'), may hold values from -3 to 3
Outputs:
- whitened: float32 [16384, 16384], P('prow', 'pcol')
The draws below stay inside these ranges and needn't reach their ends.
Inputs may be any that keep to these rules, and one draw needn't show every extreme that they name: `covariance`: entries are real-valued and of full rank.
All inputs are finite; a program needn't handle non-finite values.
Results may differ from the reference program's by a relative error of at most 0.00007.
Values sent between devices are 32-bit elements; how exact they have to be, the bound alone decides.
A program may use at most 192 MiB of HBM per device.

```python
import jax
import jax.numpy as jnp
from jax import lax

ORDER = 16384
RANK = 64
TILE = 64
N_PROW = 4
N_PCOL = 8


def draw_covariance(key, part):
    subkeys = jax.random.split(key, 3)
    positions = jnp.arange(ORDER)
    tile_row = (positions // TILE % N_PROW).astype(jnp.float32)
    tile_col = (positions // TILE % N_PCOL).astype(jnp.float32)
    row_scale = jnp.exp(tile_row / (N_PROW - 1) * jnp.log(3.0) + jax.random.uniform(subkeys[0], (ORDER,)) * jnp.log(3.3))
    col_scale = jnp.exp(tile_col / (N_PCOL - 1) * jnp.log(3.0) + jax.random.uniform(subkeys[1], (ORDER,)) * jnp.log(3.3))
    noise = jnp.clip(jax.random.normal(subkeys[2], (ORDER, ORDER), jnp.float32), -6.0, 6.0)
    return (noise * row_scale[:, None] * col_scale[None, :]).astype(jnp.float32)


def level_of(key, dims, cuts, smallest, high):
    def one(dim, parts):
        heights = jax.random.uniform(jax.random.fold_in(jax.random.fold_in(key, 6), dim), (parts,), jnp.float32, smallest / len(cuts), high / len(cuts))
        return jnp.repeat(jnp.exp(heights), dims[dim] // parts).reshape((-1,) + (1,) * (len(dims) - dim - 1))

    level = one(*cuts[0])
    for cut in cuts[1:]:
        level = level * one(*cut)
    return level


def centred(stream_key, extent, spread, reach, cuts=(), dtype=jnp.bfloat16):
    loudness = level_of(stream_key, extent, cuts, -0.22, 0.18) if cuts else 1.0
    result = jax.random.normal(stream_key, extent, jnp.float32) * spread * loudness
    return jnp.minimum(jnp.maximum(result, -reach), reach).astype(dtype)


def setup_inputs(seed: int = 0) -> dict:
    key_of = jax.random.split(jax.random.key(seed), 4)
    return {
        "covariance": draw_covariance(jax.random.fold_in(key_of[3], 71), 0),
        "factor_left": centred(key_of[1], (RANK, ORDER), 1.0, 6.0, ((1, 32),), jnp.float32),
        "factor_right": centred(key_of[2], (RANK, ORDER), 0.5, 3.0, ((0, 4), (1, 8)), jnp.float32),
    }


epsilon = 1e-06

def reference(covariance, factor_left, factor_right):
    grid_rows = N_PROW
    grid_cols = N_PCOL
    tiles_down = ORDER // (TILE * grid_rows)
    tiles_across = ORDER // (TILE * grid_cols)
    natural = factor_right.reshape(RANK, grid_cols, tiles_across, TILE).transpose(0, 2, 1, 3).reshape(RANK, ORDER)
    corrected = covariance + jnp.dot(factor_left.T, natural, precision=lax.Precision.HIGHEST, preferred_element_type=jnp.float32)
    squared = corrected * corrected
    row_mean = lax.optimization_barrier(jnp.sum(squared, axis=1)) / ORDER + epsilon
    col_mean = lax.optimization_barrier(jnp.sum(squared, axis=0)) / ORDER + epsilon
    scaled = corrected * lax.rsqrt(jnp.sqrt(row_mean[:, None] * col_mean[None, :]))
    placed = scaled.reshape(tiles_down, grid_rows, TILE, tiles_across, grid_cols, TILE)
    return placed.transpose(1, 0, 2, 4, 3, 5).reshape(ORDER, ORDER)
```

```python
import functools

import jax
import jax.numpy as jnp
from jax import lax
from jax.experimental import pallas as pl
from jax.experimental.pallas import tpu as pltpu
from jax.sharding import PartitionSpec as P

ORDER = 16384
TILE = 64


epsilon = 1e-06


def deal_columns(source):
    height = source.shape[0]
    breadth = source.shape[1]
    grid_cols = lax.axis_size("pcol")
    arranged = (
        source.reshape(height, breadth // (TILE * grid_cols), grid_cols, TILE)
        .transpose(0, 2, 1, 3)
        .reshape(height, breadth)
    )
    return lax.all_to_all(arranged, "pcol", split_axis=1, concat_axis=0, tiled=True)


def order_rows(source):
    height = source.shape[0]
    breadth = source.shape[1]
    grid_rows = lax.axis_size("prow")
    grouped = source.reshape(height // (TILE * grid_rows), grid_rows, TILE, breadth)
    return grouped.transpose(1, 0, 2, 3).reshape(height, breadth)


def body(covariance, factor_left, factor_right):
    right_panel = lax.all_gather(factor_right, "prow", axis=0, tiled=True)
    dealt = deal_columns(covariance)
    left_block = lax.all_gather(factor_left, "pcol", axis=1, tiled=True).T
    tiles_moved, left_rows = (
        lax.all_to_all(order_rows(dealt), "prow", split_axis=0, concat_axis=0, tiled=True),
        lax.all_to_all(order_rows(left_block), "prow", split_axis=0, concat_axis=0, tiled=True),
    )
    corrected = tiles_moved + jnp.dot(
        left_rows, right_panel, precision=lax.Precision.HIGHEST, preferred_element_type=jnp.float32
    )
    squared = corrected * corrected
    row_total = lax.psum(jnp.sum(squared, axis=1), "pcol")
    col_total = lax.psum(jnp.sum(squared, axis=0), "prow")
    row_mean = row_total / ORDER + epsilon
    col_mean = col_total / ORDER + epsilon
    return corrected * lax.rsqrt(jnp.sqrt(row_mean[:, None] * col_mean[None, :]))


def flip(index, size, bits):
    out, unit = 0, 1
    while unit < size:
        out = out + unit * ((index // unit + bits // unit) % 2)
        unit *= 2
    return out


def deal_kernel(grid_cols, src, dst):
    rows = src.shape[0]
    low = lax.broadcasted_iota(jnp.int32, (rows, 2 * TILE), 1) < TILE
    lanes = 2 * TILE
    for pair in range(grid_cols // 2):
        for m in range(src.shape[1] // (lanes * grid_cols)):
            at = (pair + grid_cols * m) * lanes
            first = src[:, at:at + lanes]
            at += grid_cols // 2 * lanes
            second = src[:, at:at + lanes]
            dst[0, 2 * pair, :, m * lanes:(m + 1) * lanes] = jnp.where(low, first, pltpu.roll(second, TILE, 1))
            dst[0, 2 * pair + 1, :, m * lanes:(m + 1) * lanes] = jnp.where(low, pltpu.roll(first, TILE, 1), second)


def deal(covariance, grid_rows, grid_cols):
    height, breadth = covariance.shape
    tiles = height // TILE
    step = TILE // 2
    return pl.pallas_call(
        functools.partial(deal_kernel, grid_cols),
        grid=(tiles, TILE // step),
        in_specs=[pl.BlockSpec((step, breadth), lambda j, h: (j * (TILE // step) + h, 0))],
        out_specs=pl.BlockSpec(
            (1, grid_cols, step, breadth // grid_cols),
            lambda j, h: (j % grid_rows, 0, (j // grid_rows) * (TILE // step) + h, 0),
        ),
        out_shape=jax.ShapeDtypeStruct(
            (grid_rows, grid_cols, height // grid_rows, breadth // grid_cols), jnp.float32
        ),
        compiler_params=pltpu.CompilerParams(vmem_limit_bytes=40 * 1024 * 1024),
    )(covariance)


def exchange_kernel(
    grid_rows, grid_cols, tiles, left, right, got, got_left, got_right,
    tile_send, tile_recv, left_send, left_recv, right_send, right_recv, swap_send, swap_recv, own,
):
    chips = grid_cols // 2
    p = lax.axis_index("prow")
    q = lax.axis_index("pcol")
    z, core = q // 2, q % 2
    height = tiles.shape[2]

    def target(dp, dz, dc):
        to_p = flip(p, grid_rows, dp)
        to_q = 2 * flip(z, chips, dz) + (core + dc) % 2
        return to_p, to_q

    everyone = [
        (dp, dz, dc)
        for dz in [1] + list(range(chips - 1, 1, -1)) + [0]
        for dp in range(grid_rows)
        for dc in range(2)
        if (dp, dz, dc) != (0, 0, 0)
    ]
    barrier = pltpu.get_barrier_semaphore()
    for offset in everyone:
        pl.semaphore_signal(barrier, inc=1, device_id=target(*offset), device_id_type=pl.DeviceIdType.MESH)
    pl.semaphore_wait(barrier, len(everyone))

    def copy(src, dst, send, recv, to):
        return pltpu.make_async_remote_copy(
            src_ref=src, dst_ref=dst, send_sem=send, recv_sem=recv,
            device_id=to, device_id_type=pl.DeviceIdType.MESH,
        )

    my_slot = p * grid_cols + q
    started = []
    kept = [
        pltpu.make_async_copy(left.at[p], got_left.at[core, p * chips + z], own.at[0]),
        pltpu.make_async_copy(right, got_right.at[p], own.at[1]),
    ]
    for one in kept:
        one.start()
    lefts = []
    for dz in range(chips):
        for dp in range(grid_rows):
            if (dp, dz) != (0, 0):
                n = dz * grid_rows + dp
                to = target(dp, dz, 0)
                one = copy(left.at[to[0]], got_left.at[core, p * chips + z], left_send.at[n], left_recv.at[n], to)
                one.start()
                lefts.append(one)
    for dp in range(1, grid_rows):
        one = copy(right, got_right.at[p], right_send.at[dp], right_recv.at[dp], target(dp, 0, 0))
        one.start()
        started.append(one)
    for n, offset in enumerate(everyone):
        to = target(*offset)
        one = copy(
            tiles.at[to[0], to[1]], got.at[pl.ds(pl.multiple_of(my_slot * height, height), height)],
            tile_send.at[n], tile_recv.at[n], to,
        )
        one.start()
        started.append(one)
    for one in kept:
        one.wait()
    for one in lefts:
        one.wait()
    swap = copy(got_left.at[core], got_left.at[core], swap_send, swap_recv, target(0, 0, 1))
    swap.start()

    piece = TILE // 2

    def keep(scratch, sem_in, sem_out):
        for n in range(height // piece):
            one = pltpu.make_async_copy(tiles.at[p, q, pl.ds(n * piece, piece)], scratch.at[n], sem_in.at[n])
            one.start()
        for n in range(height // piece):
            pltpu.make_async_copy(tiles.at[p, q, pl.ds(n * piece, piece)], scratch.at[n], sem_in.at[n]).wait()
            pltpu.make_async_copy(
                scratch.at[n], got.at[pl.ds(pl.multiple_of(my_slot * height + n * piece, piece), piece)], sem_out.at[n]
            ).start()
        for n in range(height // piece):
            pltpu.make_async_copy(
                scratch.at[n], got.at[pl.ds(pl.multiple_of(my_slot * height + n * piece, piece), piece)], sem_out.at[n]
            ).wait()

    pl.run_scoped(
        keep,
        pltpu.VMEM((height // piece, piece, tiles.shape[3]), jnp.float32),
        pltpu.SemaphoreType.DMA((height // piece,)),
        pltpu.SemaphoreType.DMA((height // piece,)),
    )
    swap.wait()
    for one in started:
        one.wait()


def exchange(tiles, left, right):
    grid_rows, grid_cols, height, breadth = tiles.shape
    everyone = grid_rows * grid_cols
    dma = pltpu.SemaphoreType.DMA
    anywhere = pl.BlockSpec(memory_space=pl.ANY)
    return pl.pallas_call(
        functools.partial(exchange_kernel, grid_rows, grid_cols),
        out_shape=(
            jax.ShapeDtypeStruct((everyone * height, breadth), jnp.float32),
            jax.ShapeDtypeStruct((2, everyone // 2) + left.shape[1:], jnp.float32),
            jax.ShapeDtypeStruct((grid_rows,) + right.shape, jnp.float32),
        ),
        in_specs=[anywhere] * 3,
        out_specs=(anywhere,) * 3,
        scratch_shapes=[
            dma((everyone,)), dma((everyone,)), dma((everyone // 2,)), dma((everyone // 2,)),
            dma((grid_rows,)), dma((grid_rows,)), dma, dma, dma((2,)),
        ],
        compiler_params=pltpu.CompilerParams(collective_id=0, has_side_effects=True),
    )(tiles, left, right)


def direct_body(covariance, factor_left, factor_right):
    grid_rows, grid_cols = lax.axis_size("prow"), lax.axis_size("pcol")
    rank, height = factor_left.shape
    each = height // grid_rows
    tiles = deal(covariance, grid_rows, grid_cols)
    left = (
        factor_left.reshape(rank, each // TILE, grid_rows, TILE).transpose(2, 0, 1, 3).reshape(grid_rows, rank, each)
    )
    moved, lefts, rights = exchange(tiles, left, factor_right)
    chips = grid_cols // 2
    left_rows = (
        lefts.reshape(2, grid_rows, chips, rank, each).transpose(1, 2, 0, 4, 3).reshape(-1, rank)
    )
    right_panel = rights.reshape(rank, -1)
    corrected = moved + jnp.dot(
        left_rows, right_panel, precision=lax.Precision.HIGHEST, preferred_element_type=jnp.float32
    )
    squared = corrected * corrected
    row_total = lax.psum(jnp.sum(squared, axis=1), "pcol")
    col_total = lax.psum(jnp.sum(squared, axis=0), "prow")
    row_mean = row_total / ORDER + epsilon
    col_mean = col_total / ORDER + epsilon
    return corrected * lax.rsqrt(jnp.sqrt(row_mean[:, None] * col_mean[None, :]))


def power_of_two(n):
    return n & (n - 1) == 0


def chosen(mesh, covariance):
    grid_rows, grid_cols = mesh.shape["prow"], mesh.shape["pcol"]
    tiles = covariance.shape[0] // (grid_rows * grid_cols * TILE)
    fits = tiles > 0 and tiles % grid_rows == 0 and (tiles // grid_rows) % 2 == 0
    across = covariance.shape[1] // (TILE * grid_cols)
    fits = fits and power_of_two(grid_rows) and power_of_two(grid_cols) and grid_cols > 1 and across % 2 == 0
    return direct_body if fits else body


def solution(mesh):
    placed = (P(("prow", "pcol"), None), P(None, ("prow", "pcol")), P("prow", "pcol"))

    def run(covariance, factor_left, factor_right):
        return jax.shard_map(
            chosen(mesh, covariance), mesh=mesh, in_specs=placed, out_specs=P("prow", "pcol"), check_vma=False
        )(covariance, factor_left, factor_right)

    return run
```

```python
import functools

import jax
import jax.numpy as jnp
from jax import lax
from jax.experimental import pallas as pl
from jax.experimental.pallas import tpu as pltpu
from jax.sharding import PartitionSpec as P

ORDER = 16384
TILE = 64


epsilon = 1e-06


def deal_columns(source):
    height = source.shape[0]
    breadth = source.shape[1]
    grid_cols = lax.axis_size("pcol")
    arranged = (
        source.reshape(height, breadth // (TILE * grid_cols), grid_cols, TILE)
        .transpose(0, 2, 1, 3)
        .reshape(height, breadth)
    )
    return lax.all_to_all(arranged, "pcol", split_axis=1, concat_axis=0, tiled=True)


def order_rows(source):
    height = source.shape[0]
    breadth = source.shape[1]
    grid_rows = lax.axis_size("prow")
    grouped = source.reshape(height // (TILE * grid_rows), grid_rows, TILE, breadth)
    return grouped.transpose(1, 0, 2, 3).reshape(height, breadth)


def body(covariance, factor_left, factor_right):
    right_panel = lax.all_gather(factor_right, "prow", axis=0, tiled=True)
    dealt = deal_columns(covariance)
    left_block = lax.all_gather(factor_left, "pcol", axis=1, tiled=True).T
    tiles_moved, left_rows = (
        lax.all_to_all(order_rows(dealt), "prow", split_axis=0, concat_axis=0, tiled=True),
        lax.all_to_all(order_rows(left_block), "prow", split_axis=0, concat_axis=0, tiled=True),
    )
    corrected = tiles_moved + jnp.dot(
        left_rows, right_panel, precision=lax.Precision.HIGHEST, preferred_element_type=jnp.float32
    )
    squared = corrected * corrected
    row_total = lax.psum(jnp.sum(squared, axis=1), "pcol")
    col_total = lax.psum(jnp.sum(squared, axis=0), "prow")
    row_mean = row_total / ORDER + epsilon
    col_mean = col_total / ORDER + epsilon
    return corrected * lax.rsqrt(jnp.sqrt(row_mean[:, None] * col_mean[None, :]))


def flip(index, size, bits):
    out, unit = 0, 1
    while unit < size:
        out = out + unit * ((index // unit + bits // unit) % 2)
        unit *= 2
    return out


def deal_kernel(grid_cols, src, dst):
    rows = src.shape[0]
    low = lax.broadcasted_iota(jnp.int32, (rows, 2 * TILE), 1) < TILE
    lanes = 2 * TILE
    for pair in range(grid_cols // 2):
        for m in range(src.shape[1] // (lanes * grid_cols)):
            at = (pair + grid_cols * m) * lanes
            first = src[:, at:at + lanes]
            at += grid_cols // 2 * lanes
            second = src[:, at:at + lanes]
            dst[0, 2 * pair, :, m * lanes:(m + 1) * lanes] = jnp.where(low, first, pltpu.roll(second, TILE, 1))
            dst[0, 2 * pair + 1, :, m * lanes:(m + 1) * lanes] = jnp.where(low, pltpu.roll(first, TILE, 1), second)


def deal(covariance, grid_rows, grid_cols):
    height, breadth = covariance.shape
    tiles = height // TILE
    step = TILE // 2
    return pl.pallas_call(
        functools.partial(deal_kernel, grid_cols),
        grid=(tiles, TILE // step),
        in_specs=[pl.BlockSpec((step, breadth), lambda j, h: (j * (TILE // step) + h, 0))],
        out_specs=pl.BlockSpec(
            (1, grid_cols, step, breadth // grid_cols),
            lambda j, h: (j % grid_rows, 0, (j // grid_rows) * (TILE // step) + h, 0),
        ),
        out_shape=jax.ShapeDtypeStruct(
            (grid_rows, grid_cols, height // grid_rows, breadth // grid_cols), jnp.float32
        ),
        compiler_params=pltpu.CompilerParams(vmem_limit_bytes=40 * 1024 * 1024),
    )(covariance)


def exchange_kernel(
    grid_rows, grid_cols, tiles, left, right, got, got_left, got_right,
    tile_send, tile_recv, left_send, left_recv, right_send, right_recv, swap_send, swap_recv, own,
):
    chips = grid_cols // 2
    p = lax.axis_index("prow")
    q = lax.axis_index("pcol")
    z, core = q // 2, q % 2
    height = tiles.shape[2]

    def target(dp, dz, dc):
        to_p = flip(p, grid_rows, dp)
        to_q = 2 * flip(z, chips, dz) + (core + dc) % 2
        return to_p, to_q

    def offsets(distances):
        return [
            (dp, dz, dc)
            for dp in range(grid_rows)
            for dz in distances
            for dc in range(2)
            if (dp, dz, dc) != (0, 0, 0)
        ]

    across = offsets(range(chips - 1, chips // 2 - 1, -1))
    within = offsets(range(chips // 2 - 1, -1, -1))
    beside = (z + z // 2) % 2
    everyone = [
        tuple(beside * a + (1 - beside) * b for a, b in zip(first, second))
        for first, second in zip(across + within, within + across)
    ]
    barrier = pltpu.get_barrier_semaphore()
    for offset in everyone:
        pl.semaphore_signal(barrier, inc=1, device_id=target(*offset), device_id_type=pl.DeviceIdType.MESH)
    pl.semaphore_wait(barrier, len(everyone))

    def copy(src, dst, send, recv, to):
        return pltpu.make_async_remote_copy(
            src_ref=src, dst_ref=dst, send_sem=send, recv_sem=recv,
            device_id=to, device_id_type=pl.DeviceIdType.MESH,
        )

    my_slot = p * grid_cols + q
    started = []
    kept = [
        pltpu.make_async_copy(left.at[p], got_left.at[core, p * chips + z], own.at[0]),
        pltpu.make_async_copy(right, got_right.at[p], own.at[1]),
    ]
    for one in kept:
        one.start()
    lefts = []
    for dz in range(chips):
        for dp in range(grid_rows):
            if (dp, dz) != (0, 0):
                n = dz * grid_rows + dp
                to = target(dp, dz, 0)
                one = copy(left.at[to[0]], got_left.at[core, p * chips + z], left_send.at[n], left_recv.at[n], to)
                one.start()
                lefts.append(one)
    for dp in range(1, grid_rows):
        one = copy(right, got_right.at[p], right_send.at[dp], right_recv.at[dp], target(dp, 0, 0))
        one.start()
        started.append(one)
    for n, offset in enumerate(everyone):
        to = target(*offset)
        slot = (offset[0] * chips + offset[1]) * 2 + offset[2]
        one = copy(
            tiles.at[to[0], to[1]], got.at[pl.ds(pl.multiple_of(my_slot * height, height), height)],
            tile_send.at[n], tile_recv.at[slot], to,
        )
        one.start()
        started.append(one)
    for one in kept:
        one.wait()
    for one in lefts:
        one.wait()
    swap = copy(got_left.at[core], got_left.at[core], swap_send, swap_recv, target(0, 0, 1))
    swap.start()

    piece = TILE // 2

    def keep(scratch, sem_in, sem_out):
        for n in range(height // piece):
            one = pltpu.make_async_copy(tiles.at[p, q, pl.ds(n * piece, piece)], scratch.at[n], sem_in.at[n])
            one.start()
        for n in range(height // piece):
            pltpu.make_async_copy(tiles.at[p, q, pl.ds(n * piece, piece)], scratch.at[n], sem_in.at[n]).wait()
            pltpu.make_async_copy(
                scratch.at[n], got.at[pl.ds(pl.multiple_of(my_slot * height + n * piece, piece), piece)], sem_out.at[n]
            ).start()
        for n in range(height // piece):
            pltpu.make_async_copy(
                scratch.at[n], got.at[pl.ds(pl.multiple_of(my_slot * height + n * piece, piece), piece)], sem_out.at[n]
            ).wait()

    pl.run_scoped(
        keep,
        pltpu.VMEM((height // piece, piece, tiles.shape[3]), jnp.float32),
        pltpu.SemaphoreType.DMA((height // piece,)),
        pltpu.SemaphoreType.DMA((height // piece,)),
    )
    swap.wait()
    for one in started:
        one.wait()


def exchange(tiles, left, right):
    grid_rows, grid_cols, height, breadth = tiles.shape
    everyone = grid_rows * grid_cols
    dma = pltpu.SemaphoreType.DMA
    anywhere = pl.BlockSpec(memory_space=pl.ANY)
    return pl.pallas_call(
        functools.partial(exchange_kernel, grid_rows, grid_cols),
        out_shape=(
            jax.ShapeDtypeStruct((everyone * height, breadth), jnp.float32),
            jax.ShapeDtypeStruct((2, everyone // 2) + left.shape[1:], jnp.float32),
            jax.ShapeDtypeStruct((grid_rows,) + right.shape, jnp.float32),
        ),
        in_specs=[anywhere] * 3,
        out_specs=(anywhere,) * 3,
        scratch_shapes=[
            dma((everyone,)), dma((everyone,)), dma((everyone // 2,)), dma((everyone // 2,)),
            dma((grid_rows,)), dma((grid_rows,)), dma, dma, dma((2,)),
        ],
        compiler_params=pltpu.CompilerParams(collective_id=0, has_side_effects=True),
    )(tiles, left, right)


def direct_body(covariance, factor_left, factor_right):
    grid_rows, grid_cols = lax.axis_size("prow"), lax.axis_size("pcol")
    rank, height = factor_left.shape
    each = height // grid_rows
    tiles = deal(covariance, grid_rows, grid_cols)
    left = (
        factor_left.reshape(rank, each // TILE, grid_rows, TILE).transpose(2, 0, 1, 3).reshape(grid_rows, rank, each)
    )
    moved, lefts, rights = exchange(tiles, left, factor_right)
    chips = grid_cols // 2
    left_rows = (
        lefts.reshape(2, grid_rows, chips, rank, each).transpose(1, 2, 0, 4, 3).reshape(-1, rank)
    )
    right_panel = rights.reshape(rank, -1)
    corrected = moved + jnp.dot(
        left_rows, right_panel, precision=lax.Precision.HIGH, preferred_element_type=jnp.float32
    )
    squared = corrected * corrected
    row_total = lax.psum(jnp.sum(squared, axis=1), "pcol")
    col_total = lax.psum(jnp.sum(squared, axis=0), "prow")
    row_mean = row_total / ORDER + epsilon
    col_mean = col_total / ORDER + epsilon
    return corrected * lax.rsqrt(jnp.sqrt(row_mean[:, None] * col_mean[None, :]))


def power_of_two(n):
    return n & (n - 1) == 0


def chosen(mesh, covariance):
    grid_rows, grid_cols = mesh.shape["prow"], mesh.shape["pcol"]
    tiles = covariance.shape[0] // (grid_rows * grid_cols * TILE)
    fits = tiles > 0 and tiles % grid_rows == 0 and (tiles // grid_rows) % 2 == 0
    across = covariance.shape[1] // (TILE * grid_cols)
    fits = fits and power_of_two(grid_rows) and power_of_two(grid_cols) and grid_cols > 1 and across % 2 == 0
    return direct_body if fits else body


def solution(mesh):
    placed = (P(("prow", "pcol"), None), P(None, ("prow", "pcol")), P("prow", "pcol"))

    def run(covariance, factor_left, factor_right):
        return jax.shard_map(
            chosen(mesh, covariance), mesh=mesh, in_specs=placed, out_specs=P("prow", "pcol"), check_vma=False
        )(covariance, factor_left, factor_right)

    return run
```
